32 devices in a mesh: mem: 4 (over x, core), lat: 8 (over z, y).
Axes of the slice: x: 2, y: 2, z: 4, core: 2. Of those that a mesh axis runs over, the one named last changes fastest.
Arguments:
- control: bfloat16 [8, 10, 704, 1440], P('mem', None, 'lat'), may hold values from -6 to 6
- perturb: bfloat16 [8, 10, 704, 1440], P('mem', None, None, 'lat'), may hold values from -6 to 6
- lon_loc: bfloat16 [1440, 1440], P(None, 'mem'), may hold values from 0 to 1, as said below
- lat_loc: bfloat16 [704, 704], P('mem'), may hold values from 0 to 1, as said below
- static_scale: float32 [10, 704, 1440], P(None, 'mem', 'lat'), may hold values from 0.3 to 1
- static_field: float32 [10, 704, 1440], P(None, 'mem', 'lat'), may hold values from -6 to 6
- courant: float32 [2, 704, 1440], P(None, 'mem', 'lat'), may hold values from -0.48 to 0.48
Outputs:
- increment: float32 [10, 704, 1440], P(None, 'mem', 'lat')
- evolved: float32 [10, 704, 1440], P(None, 'mem', 'lat')
The draws below stay inside these ranges and needn't reach their ends.
Inputs may be any that keep to these rules, and one draw needn't show every extreme that they name: `lon_loc`: Symmetric, with positive entries. `lat_loc`: Symmetric, with positive entries.
All inputs are finite; a program needn't handle non-finite values.
Results may differ from the reference program's by a relative error of at most 0.0027.
Values may be sent and summed in bfloat16 or wider, within the bound.
No kernel may reach another device: no remote copies, remote signals or barrier semaphores. Data moves between devices by JAX's collectives and lax.ppermute only.
A program may use at most 128 MiB of HBM per device.

```python
import math
import jax
import jax.numpy as jnp
from jax import lax

MEMBERS = 8
FIELDS = 10
NLAT = 704
NLON = 1440
STEPS = 4


def gaussian_taper(key, amount, periodic):
    cells = jnp.arange(amount, dtype=jnp.int32)
    distance = jnp.abs(cells[:, None] - cells[None, :])
    if periodic:
        distance = jnp.minimum(distance, amount - distance)
    length = amount / 32.0
    floor_level = 0.15
    spacing = distance.astype(jnp.float32)
    envelope = floor_level + (1.0 - floor_level) * jnp.exp(-(spacing * spacing) / (2.0 * length * length))
    modulation = jax.random.uniform(key, (amount, amount), jnp.float32, 0.5, 1.5)
    symmetric = 0.5 * (modulation + modulation.T)
    normalizer = jnp.sqrt(amount * floor_level * floor_level + length * 1.7725)
    return (envelope * symmetric / normalizer).astype(jnp.bfloat16)


def draw_lon_loc(key, part):
    return gaussian_taper(jax.random.fold_in(key, 11), NLON, True)


def draw_lat_loc(key, part):
    return gaussian_taper(jax.random.fold_in(key, 23), NLAT, False)


def raised(array, rng, source, target, blocks, factor):
    def block_of(position):
        return (jnp.arange(array.shape[position]) // (array.shape[position] // blocks)).reshape((-1,) + (1,) * (array.ndim - 1 - position))

    first = jax.random.permutation(rng, blocks)[block_of(target)]
    far = (block_of(target) + blocks // 2) % blocks
    return jnp.where((block_of(source) == first) | (block_of(source) == far), factor * array, array)


def steps_of(key, extent, shards, least, largest):
    loudness = 1.0
    for dim, parts in shards:
        heights = jax.random.uniform(jax.random.fold_in(jax.random.fold_in(key, 6), dim), (parts,), jnp.float32, least / len(shards), largest / len(shards))
        loudness = loudness * jnp.repeat(jnp.exp(heights), extent[dim] // parts).reshape((-1,) + (1,) * (len(extent) - 1 - dim))
    return loudness


def scatter_about(own_key, extent, scale, bound, cuts=(), held_as=jnp.bfloat16):
    values = jax.random.normal(own_key, extent, jnp.float32) * scale
    if len(cuts) > 0:
        values = steps_of(own_key, extent, cuts, -0.22, 0.18) * values
    return jnp.clip(values, min=-bound, max=bound).astype(held_as)


def gaussian_with(rng, dims, spread, limit, shards, heavy, held_as=jnp.bfloat16):
    entries = spread * jax.random.normal(rng, dims, jnp.float32)
    if shards:
        entries = entries * steps_of(rng, dims, shards, -0.22, 0.18)
    return jnp.clip(raised(entries, jax.random.fold_in(rng, 3), *heavy), -limit, limit).astype(held_as)


def setup_inputs(seed: int = 0) -> dict:
    arg_keys = jax.random.split(jax.random.key(seed), 8)
    return {
        "control": scatter_about(arg_keys[0], (MEMBERS, FIELDS, NLAT, NLON), 1.0, 6.0, ((0, 4), (2, 8))),
        "perturb": gaussian_with(arg_keys[1], (MEMBERS, FIELDS, NLAT, NLON), 1.0, 6.0, ((0, 4), (3, 8)), (0, 2, 4, 2.0)),
        "lon_loc": draw_lon_loc(jax.random.fold_in(arg_keys[7], 71), 0),
        "lat_loc": draw_lat_loc(jax.random.fold_in(arg_keys[7], 71), 0),
        "static_scale": jnp.clip(jnp.exp(math.log(1.0) - 1.2039728 * jax.random.uniform(arg_keys[4], (FIELDS, NLAT, NLON), jnp.float32) ** steps_of(arg_keys[4], (FIELDS, NLAT, NLON), ((1, 4), (2, 8)), -0.2, 0.2)), 0.3, 1.0),
        "static_field": scatter_about(arg_keys[5], (FIELDS, NLAT, NLON), 1.0, 6.0, ((1, 4), (2, 8)), jnp.float32),
        "courant": jnp.clip(jax.random.uniform(arg_keys[6], (2, NLAT, NLON), jnp.float32, -0.48, 0.48) * steps_of(arg_keys[6], (2, NLAT, NLON), ((1, 4), (2, 8)), -0.4, 0.0), -0.48, 0.48),
    }


def upwind(padded, east_west, north_south):
    center = padded[:, 1:-1, 1:-1]
    western = padded[:, 1:-1, :-2]
    eastern = padded[:, 1:-1, 2:]
    southern = padded[:, :-2, 1:-1]
    northern = padded[:, 2:, 1:-1]
    zonal = jnp.maximum(east_west, 0.0) * (center - western) + jnp.minimum(east_west, 0.0) * (eastern - center)
    meridional = jnp.maximum(north_south, 0.0) * (center - southern) + jnp.minimum(north_south, 0.0) * (northern - center)
    return center - zonal - meridional

def advance(current, courant):
    for step_index in range(STEPS):
        padded = jnp.pad(current, ((0, 0), (1, 1), (0, 0)))
        padded = jnp.concatenate([padded[:, :, -1:], padded, padded[:, :, :1]], axis=2)
        current = upwind(padded, courant[0], courant[1])
    return current

def reference(control, perturb, lon_loc, lat_loc, static_scale, static_field, courant):
    members = control.shape[0]
    fields = control.shape[1]
    lon_full = lon_loc.astype(jnp.float32)
    lat_full = lat_loc.astype(jnp.float32)

    def add_member(total, pair):
        control_one, perturb_one = pair
        flat = control_one.astype(jnp.float32).reshape(fields * NLAT, NLON)
        along_lon = jnp.dot(flat, lon_full, precision=lax.Precision.HIGHEST)
        along_lon = along_lon.astype(jnp.bfloat16).astype(jnp.float32).reshape(fields, NLAT, NLON)
        localized = jnp.einsum('ab,fbl->fal', lat_full, along_lon, precision=lax.Precision.HIGHEST)
        return (total + localized * perturb_one.astype(jnp.float32), None)
    total, unused = lax.scan(add_member, jnp.zeros((fields, NLAT, NLON), jnp.float32), (control, perturb))
    ensemble = total * (1.0 / math.sqrt(members - 1))
    increment = ensemble + static_scale * static_field
    evolved = advance(increment, courant)
    return (increment, evolved)
```

```python
import functools
import math

import jax
import jax.numpy as jnp
from jax import lax
from jax.experimental import pallas as pl
from jax.experimental.pallas import tpu as pltpu
from jax.sharding import PartitionSpec as P

STEPS = 4
LANES = 128
HALF = 64
ANY = pl.ANY
SMEM = pltpu.SMEM
VMEM = pltpu.VMEM


def padded_2(shard, sides, width, wrap):
    for axis, dim in sides:
        size, length = (lax.axis_size(axis), shard.shape[dim])
        up = [(i, (i + 1) % size) for i in range(size if wrap else size - 1)]
        down = [(j, i) for i, j in up]
        last = lax.slice_in_dim(shard, length - width, length, axis=dim)
        leading = lax.slice_in_dim(shard, 0, width, axis=dim)
        before = lax.ppermute(last, axis, up)
        after = lax.ppermute(leading, axis, down)
        shard = jnp.concatenate([before, shard, after], axis=dim)
    return shard


def upwind(padded, east_west, north_south):
    center = padded[:, 1:-1, 1:-1]
    western = padded[:, 1:-1, :-2]
    eastern = padded[:, 1:-1, 2:]
    southern = padded[:, :-2, 1:-1]
    northern = padded[:, 2:, 1:-1]
    zonal = jnp.maximum(east_west, 0.0) * (center - western) + jnp.minimum(east_west, 0.0) * (
        eastern - center
    )
    meridional = jnp.maximum(north_south, 0.0) * (center - southern) + jnp.minimum(
        north_south, 0.0
    ) * (northern - center)
    return center - zonal - meridional


def evolve(current, courant):
    fields = current.shape[0]
    stacked = jnp.concatenate([current, courant], axis=0)
    extended = padded_2(stacked, (("lat", 2),), STEPS, True)
    extended = padded_2(extended, (("mem", 1),), STEPS, False)
    result = extended[:fields]
    wind_ext = extended[fields:]
    for step_index in range(STEPS):
        margin = step_index + 1
        inner_wind = wind_ext[
            :, margin : wind_ext.shape[1] - margin, margin : wind_ext.shape[2] - margin
        ]
        result = upwind(result, inner_wind[0], inner_wind[1])
    return result


def per_device_any(control, perturb, lon_loc, lat_loc, static_scale, static_field, courant):
    along_lon = jnp.einsum(
        "mfal,lc->amfc",
        control,
        lax.all_gather(lon_loc, "mem", axis=1, tiled=True),
        preferred_element_type=jnp.float32,
    ).astype(jnp.bfloat16)
    banded = lax.all_to_all(along_lon, "lat", split_axis=3, concat_axis=0, tiled=True)
    nlat = banded.shape[0]
    mem_here = banded.shape[1]
    fields = banded.shape[2]
    lon_width = banded.shape[3]
    flat_band = banded.reshape(nlat, mem_here * fields * lon_width)
    pert_rows = jnp.transpose(perturb, (2, 0, 1, 3))
    lat_weights_all = lax.all_gather(lat_loc, "mem", axis=0, tiled=True)
    members = mem_here * lax.axis_size("mem")
    ens_scale = 1.0 / math.sqrt(members - 1)
    rows_own = nlat // lax.axis_size("mem")
    localized = jnp.dot(lat_weights_all, flat_band, preferred_element_type=jnp.float32)
    localized = localized.reshape(nlat, mem_here, fields, lon_width)
    ensemble_all = jnp.transpose(
        lax.psum(jnp.sum(localized * pert_rows.astype(jnp.float32), axis=1) * ens_scale, "mem"),
        (1, 0, 2),
    )
    offset = lax.axis_index("mem") * rows_own
    ensemble = lax.dynamic_slice_in_dim(ensemble_all, offset, rows_own, 1)
    increment = ensemble + static_scale * static_field
    evolved = evolve(increment, courant)
    return (increment, evolved)


def xor_permute(value, axis, mask):
    return lax.ppermute(value, axis, [(i, i ^ mask) for i in range(lax.axis_size(axis))])


def copy_all(pairs, sems):
    copies = [pltpu.make_async_copy(a, b, sems.at[i]) for i, (a, b) in enumerate(pairs)]
    for c in copies:
        c.start()
    return copies


def spread_matrix(rows, width, shift):
    k = lax.broadcasted_iota(jnp.int32, (rows, 2 * LANES), 0)
    n = lax.broadcasted_iota(jnp.int32, (rows, 2 * LANES), 1)
    n = jnp.where(n >= LANES + HALF, n - HALF, n)
    return jnp.where((n < width) & (k == n + shift), 1.0, 0.0).astype(jnp.bfloat16)


def spread_body(width, bands, mem_ref, *refs):
    slabs = refs[:-3]
    out, held, sems = refs[-3:]
    here = mem_ref[0]
    copies = copy_all([(s, held.at[here ^ r]) for r, s in enumerate(slabs)], sems)
    for c in copies:
        c.wait()
    picks = [spread_matrix(held.shape[2], width, h * width) for h in range(bands)]

    def slab(q, carry):
        for h in range(bands):
            out[q * bands + h] = jnp.dot(
                held[q], picks[h], preferred_element_type=jnp.float32
            ).astype(jnp.bfloat16)
        return carry

    lax.fori_loop(0, len(slabs), slab, 0)


def spread_weights(slabs, width, bands, mem_index):
    rows, cols = slabs[0].shape
    return pl.pallas_call(
        functools.partial(spread_body, width, bands),
        out_shape=jax.ShapeDtypeStruct((len(slabs) * bands, rows, 2 * LANES), jnp.bfloat16),
        in_specs=[pl.BlockSpec(memory_space=SMEM)] + [pl.BlockSpec(memory_space=ANY)] * len(slabs),
        out_specs=pl.BlockSpec(memory_space=VMEM),
        scratch_shapes=[
            VMEM((len(slabs), rows, cols), jnp.bfloat16),
            pltpu.SemaphoreType.DMA((len(slabs),)),
        ],
        name="spread_weights",
    )(mem_index, *slabs)


def lon_body(masks, first, pairs, rows, lat_ref, control, weights, *refs):
    outs = refs[: len(masks)]
    fields_here, held, sems = refs[len(masks) :]
    here = lat_ref[0]
    members = control.shape[0]
    source = control.at[:, pl.ds(first * rows, 2 * pairs * rows), :]
    copies = copy_all(
        [(source, fields_here)]
        + [(weights.at[here ^ s], held.at[i]) for i, s in enumerate(masks)],
        sems,
    )
    copies[0].wait()
    low = lax.broadcasted_iota(jnp.int32, (rows, LANES), 1) < HALF
    for i, out in enumerate(outs):
        copies[1 + i].wait()
        for m in range(members):
            acc = jnp.dot(fields_here[m], held[i], preferred_element_type=jnp.float32)
            for p in range(pairs):
                one = acc[2 * p * rows : (2 * p + 1) * rows]
                two = acc[(2 * p + 1) * rows : (2 * p + 2) * rows]
                out[p, m, 0] = one[:, :LANES].astype(jnp.bfloat16)
                out[p, m, 1] = two[:, :LANES].astype(jnp.bfloat16)
                out[p, m, 2] = jnp.where(low, one[:, LANES:], two[:, LANES:]).astype(jnp.bfloat16)


def lon_blocks(control, weights, lat_index, masks, first, pairs, rows):
    members, _, nlon = control.shape
    block = jax.ShapeDtypeStruct((pairs, members, 3, rows, LANES), jnp.bfloat16)
    flops = 2 * members * 2 * pairs * rows * nlon * 2 * LANES * len(masks)
    return pl.pallas_call(
        functools.partial(lon_body, masks, first, pairs, rows),
        out_shape=[block] * len(masks),
        in_specs=[
            pl.BlockSpec(memory_space=SMEM),
            pl.BlockSpec(memory_space=ANY),
            pl.BlockSpec(memory_space=ANY),
        ],
        out_specs=[pl.BlockSpec(memory_space=VMEM)] * len(masks),
        scratch_shapes=[
            VMEM((members, 2 * pairs * rows, nlon), jnp.bfloat16),
            VMEM((len(masks), nlon, 2 * LANES), jnp.bfloat16),
            pltpu.SemaphoreType.DMA((1 + len(masks),)),
        ],
        cost_estimate=pl.CostEstimate(
            flops=flops, transcendentals=0, bytes_accessed=len(masks) * nlon * 4 * LANES
        ),
        name="lon_blocks",
    )(lat_index, control, weights)


def lat_body(first, pairs, width, scale, n_lat, n_mem, lat_ref, mem_ref, *refs):
    blocks = refs[:n_lat]
    slabs = refs[n_lat : n_lat + n_mem]
    perturb = refs[n_lat + n_mem]
    outs = refs[n_lat + n_mem + 1 : n_lat + 2 * n_mem + 1]
    weights, banded, pert, total, sems, pair_sems = refs[n_lat + 2 * n_mem + 1 :]
    here = lat_ref[0]
    mem_here = mem_ref[0]
    rows = blocks[0].shape[3]
    rows_own = slabs[0].shape[0]
    members = pert.shape[0]
    copies = copy_all(
        [
            (b, banded.at[:, :, :, pl.ds(pl.multiple_of((here ^ s) * rows, 8), rows), :])
            for s, b in enumerate(blocks)
        ]
        + [
            (w, weights.at[pl.ds(pl.multiple_of((mem_here ^ r) * rows_own, 8), rows_own), :])
            for r, w in enumerate(slabs)
        ],
        sems,
    )
    pair_copies = copy_all(
        [
            (perturb.at[:, pl.ds(first + 2 * p, 2)], pert.at[:, pl.ds(2 * p, 2)])
            for p in range(pairs)
        ],
        pair_sems,
    )
    for c in copies:
        c.wait()
    for c in pair_copies:
        c.wait()
    edge = width - LANES
    k = lax.broadcasted_iota(jnp.int32, (width, LANES), 0)
    n = lax.broadcasted_iota(jnp.int32, (width, LANES), 1)
    picks = [
        jnp.where((k == n - h * HALF + LANES) & (n >= h * HALF), 1.0, 0.0).astype(jnp.bfloat16)
        for h in range(2)
    ]

    def pair(p, carry):
        for t in range(3):
            both = jnp.concatenate([banded[p, m, t] for m in range(members)], axis=1)
            local = jnp.dot(weights[...], both, preferred_element_type=jnp.float32)
            acc = None
            for m in range(members):
                if t < 2:
                    factor = pert[m, 2 * p + t, :, :LANES].astype(jnp.float32)
                else:
                    factor = jnp.dot(
                        pert[m, 2 * p], picks[0], preferred_element_type=jnp.float32
                    ) + jnp.dot(pert[m, 2 * p + 1], picks[1], preferred_element_type=jnp.float32)
                term = local[:, m * LANES : (m + 1) * LANES] * factor
                acc = term if acc is None else acc + term
            total[...] = acc * scale
            for r in range(n_mem):
                part = total[pl.ds(pl.multiple_of((mem_here ^ r) * rows_own, 8), rows_own), :]
                outs[r][p, t] = part.astype(outs[r].dtype)
        return carry

    lax.fori_loop(0, pairs, pair, 0)


def lat_products(blocks, slabs, perturb, lat_index, mem_index, first, scale):
    pairs, members, _, rows, _ = blocks[0].shape
    n_lat, n_mem = len(blocks), len(slabs)
    rows_own, nlat = slabs[0].shape
    width = perturb.shape[3]
    own = jax.ShapeDtypeStruct((pairs, 3, rows_own, LANES), jnp.float32)
    sent = jax.ShapeDtypeStruct((pairs, 3, rows_own, LANES), jnp.bfloat16)
    return pl.pallas_call(
        functools.partial(lat_body, first, pairs, width, scale, n_lat, n_mem),
        out_shape=[own] + [sent] * (n_mem - 1),
        in_specs=[pl.BlockSpec(memory_space=SMEM)] * 2
        + [pl.BlockSpec(memory_space=ANY)] * (n_lat + n_mem + 1),
        out_specs=[pl.BlockSpec(memory_space=VMEM)] * n_mem,
        scratch_shapes=[
            VMEM((nlat, nlat), jnp.bfloat16),
            VMEM((pairs, members, 3, nlat, LANES), jnp.bfloat16),
            VMEM((members, 2 * pairs, nlat, width), jnp.bfloat16),
            VMEM((nlat, LANES), jnp.float32),
            pltpu.SemaphoreType.DMA((n_lat + n_mem,)),
            pltpu.SemaphoreType.DMA((pairs,)),
        ],
        cost_estimate=pl.CostEstimate(
            flops=2 * nlat * nlat * members * pairs * 3 * LANES,
            transcendentals=0,
            bytes_accessed=members * 2 * pairs * nlat * 4 * width,
        ),
        name="lat_products",
    )(lat_index, mem_index, *blocks, *slabs, perturb)


def sum_body(chunks, n_mem, *refs):
    parts = refs[: len(chunks) * n_mem]
    scale, field, out = refs[len(chunks) * n_mem :]
    width = out.shape[2]
    edge = width - LANES
    for c, (first, pairs) in enumerate(chunks):
        mine = parts[c * n_mem : (c + 1) * n_mem]

        def pair(p, carry):
            tiles = []
            for t in range(3):
                acc = mine[0][p, t]
                for part in mine[1:]:
                    acc = acc + part[p, t].astype(jnp.float32)
                tiles.append(acc)
            tails = [tiles[2], pltpu.roll(tiles[2], HALF, 1)]
            for h in range(2):
                f = first + 2 * p + h
                background = scale[f] * field[f]
                out[f, :, :LANES] = tiles[h] + background[:, :LANES]
                out[f, :, LANES:] = tails[h][:, :edge] + background[:, LANES:]
            return carry

        lax.fori_loop(0, pairs, pair, 0)


def sum_parts(parts, chunks, n_mem, static_scale, static_field):
    return pl.pallas_call(
        functools.partial(sum_body, chunks, n_mem),
        out_shape=jax.ShapeDtypeStruct(static_scale.shape, jnp.float32),
        in_specs=[pl.BlockSpec(memory_space=VMEM)] * (len(parts) + 2),
        out_specs=pl.BlockSpec(memory_space=VMEM),
        name="sum_parts",
    )(*parts, static_scale, static_field)


def chunks_of(fields):
    plan, first = ([], 0)
    left = fields // 2
    while left:
        pairs = min(2, left)
        plan.append((first, pairs))
        first, left = (first + 2 * pairs, left - pairs)
    return plan


def per_device_banded(control, perturb, lon_loc, lat_loc, static_scale, static_field, courant):
    n_mem, n_lat = (lax.axis_size("mem"), lax.axis_size("lat"))
    members, fields, rows, nlon = control.shape
    width = perturb.shape[3]
    mem_index = lax.axis_index("mem").astype(jnp.int32).reshape(1)
    lat_index = lax.axis_index("lat").astype(jnp.int32).reshape(1)
    scale = 1.0 / math.sqrt(members * n_mem - 1)
    chunks = chunks_of(fields)

    lon_slabs = [lon_loc]
    lat_slabs = [lat_loc]
    step = 1
    order = []
    lon_by_mask = {0: lon_loc}
    for bit in reversed(range(n_mem.bit_length() - 1)):
        for have in list(lon_by_mask):
            lon_by_mask[have ^ (1 << bit)] = xor_permute(lon_by_mask[have], "mem", 1 << bit)
    lon_slabs = [lon_by_mask[r] for r in range(n_mem)]
    lat_slabs = [lat_loc] + [xor_permute(lat_loc, "mem", r) for r in range(1, n_mem)]
    weights = spread_weights(lon_slabs, width, n_lat // n_mem, mem_index)

    flat = control.reshape(members, fields * rows, nlon)
    far = [s for s in (6, 7, 4, 5, 2, 3, 1, 0)]
    received = []
    for first, pairs in chunks:
        blocks = lon_blocks(flat, weights, lat_index, tuple(far), first, pairs, rows)
        by_mask = dict(zip(far, blocks))
        received.append(
            [by_mask[0]]
            + [None] * (n_lat - 1)
        )
        for s in far:
            if s:
                received[-1][s] = xor_permute(by_mask[s], "lat", s)
    parts = []
    for (first, pairs), blocks in zip(chunks, received):
        made = lat_products(blocks, lat_slabs, perturb, lat_index, mem_index, first, scale)
        parts.append(made[0])
        parts.extend(xor_permute(made[r], "mem", r) for r in range(1, n_mem))
    increment = sum_parts(parts, chunks, n_mem, static_scale, static_field)
    evolved = evolve(increment, courant)
    return (increment, evolved)


def per_device(control, perturb, *rest):
    n_mem, n_lat = (lax.axis_size("mem"), lax.axis_size("lat"))
    rows = control.shape[2]
    width = perturb.shape[3]
    nlat = perturb.shape[2]
    banded = (
        LANES < width <= LANES + HALF
        and rows % 8 == 0
        and (nlat // n_mem) % 8 == 0
        and control.shape[1] % 2 == 0
        and n_lat == 8
        and n_lat % n_mem == 0
    )
    return (per_device_banded if banded else per_device_any)(control, perturb, *rest)


def solution(mesh):
    placed = (
        P("mem", None, "lat", None),
        P("mem", None, None, "lat"),
        P(None, "mem"),
        P("mem", None),
        P(None, "mem", "lat"),
        P(None, "mem", "lat"),
        P(None, "mem", "lat"),
    )
    return jax.shard_map(
        per_device,
        mesh=mesh,
        in_specs=placed,
        out_specs=(P(None, "mem", "lat"), P(None, "mem", "lat")),
        check_vma=False,
    )
```

```python
import functools
import math

import jax
import jax.numpy as jnp
from jax import lax
from jax.experimental import pallas as pl
from jax.experimental.pallas import tpu as pltpu
from jax.sharding import PartitionSpec as P


STEPS = 4
LANES = 128
HALF = 64
HALO = 8
ANY = pl.ANY
SMEM = pltpu.SMEM
VMEM = pltpu.VMEM


def padded_2(shard, sides, width, wrap):
    for axis, dim in sides:
        size, length = (lax.axis_size(axis), shard.shape[dim])
        up = [(i, (i + 1) % size) for i in range(size if wrap else size - 1)]
        down = [(j, i) for i, j in up]
        last = lax.slice_in_dim(shard, length - width, length, axis=dim)
        leading = lax.slice_in_dim(shard, 0, width, axis=dim)
        before = lax.ppermute(last, axis, up)
        after = lax.ppermute(leading, axis, down)
        shard = jnp.concatenate([before, shard, after], axis=dim)
    return shard


def upwind(padded, east_west, north_south):
    center = padded[:, 1:-1, 1:-1]
    western = padded[:, 1:-1, :-2]
    eastern = padded[:, 1:-1, 2:]
    southern = padded[:, :-2, 1:-1]
    northern = padded[:, 2:, 1:-1]
    zonal = jnp.maximum(east_west, 0.0) * (center - western) + jnp.minimum(east_west, 0.0) * (
        eastern - center
    )
    meridional = jnp.maximum(north_south, 0.0) * (center - southern) + jnp.minimum(
        north_south, 0.0
    ) * (northern - center)
    return center - zonal - meridional


def evolve(current, courant):
    fields = current.shape[0]
    stacked = jnp.concatenate([current, courant], axis=0)
    extended = padded_2(stacked, (("lat", 2),), STEPS, True)
    extended = padded_2(extended, (("mem", 1),), STEPS, False)
    result = extended[:fields]
    wind_ext = extended[fields:]
    for step_index in range(STEPS):
        margin = step_index + 1
        inner_wind = wind_ext[
            :, margin : wind_ext.shape[1] - margin, margin : wind_ext.shape[2] - margin
        ]
        result = upwind(result, inner_wind[0], inner_wind[1])
    return result


def per_device_any(control, perturb, lon_loc, lat_loc, static_scale, static_field, courant):
    along_lon = jnp.einsum(
        "mfal,lc->amfc",
        control,
        lax.all_gather(lon_loc, "mem", axis=1, tiled=True),
        preferred_element_type=jnp.float32,
    ).astype(jnp.bfloat16)
    banded = lax.all_to_all(along_lon, "lat", split_axis=3, concat_axis=0, tiled=True)
    nlat = banded.shape[0]
    mem_here = banded.shape[1]
    fields = banded.shape[2]
    lon_width = banded.shape[3]
    flat_band = banded.reshape(nlat, mem_here * fields * lon_width)
    pert_rows = jnp.transpose(perturb, (2, 0, 1, 3))
    lat_weights_all = lax.all_gather(lat_loc, "mem", axis=0, tiled=True)
    members = mem_here * lax.axis_size("mem")
    ens_scale = 1.0 / math.sqrt(members - 1)
    rows_own = nlat // lax.axis_size("mem")
    localized = jnp.dot(lat_weights_all, flat_band, preferred_element_type=jnp.float32)
    localized = localized.reshape(nlat, mem_here, fields, lon_width)
    ensemble_all = jnp.transpose(
        lax.psum(jnp.sum(localized * pert_rows.astype(jnp.float32), axis=1) * ens_scale, "mem"),
        (1, 0, 2),
    )
    offset = lax.axis_index("mem") * rows_own
    ensemble = lax.dynamic_slice_in_dim(ensemble_all, offset, rows_own, 1)
    increment = ensemble + static_scale * static_field
    evolved = evolve(increment, courant)
    return (increment, evolved)


def xor_permute(value, axis, mask):
    return lax.ppermute(value, axis, [(i, i ^ mask) for i in range(lax.axis_size(axis))])


def copy_all(pairs, sems):
    copies = [pltpu.make_async_copy(a, b, sems.at[i]) for i, (a, b) in enumerate(pairs)]
    for c in copies:
        c.start()
    return copies


def spread_matrix(rows, width, shift):
    k = lax.broadcasted_iota(jnp.int32, (rows, 2 * LANES), 0)
    n = lax.broadcasted_iota(jnp.int32, (rows, 2 * LANES), 1)
    n = jnp.where(n >= LANES + HALF, n - HALF, n)
    late = n >= LANES + HALF - STEPS
    column = jnp.where(late, n - LANES - HALF, n) + shift
    taken = late | (n < width + STEPS)
    return jnp.where(taken & (k == column), 1.0, 0.0).astype(jnp.bfloat16)


def spread_body(width, bands, mem_ref, *refs):
    slabs = refs[:-3]
    out, held, sems = refs[-3:]
    here = mem_ref[0]
    copies = copy_all([(s, held.at[here ^ r]) for r, s in enumerate(slabs)], sems)
    for c in copies:
        c.wait()
    count, _, cols = held.shape
    picks = [spread_matrix(cols, width, h * width) for h in range(bands)]
    tail = (cols - STEPS) // LANES * LANES
    pick_last = spread_matrix(cols - tail, width, cols - tail)
    pick_first = spread_matrix(LANES, width, (bands - 1) * width - cols)

    def slab(q, carry):
        before = held[(q + count - 1) % count, :, tail:]
        after = held[(q + 1) % count, :, :LANES]
        for h in range(bands):
            acc = jnp.dot(held[q], picks[h], preferred_element_type=jnp.float32)
            if h == 0:
                acc += jnp.dot(before, pick_last, preferred_element_type=jnp.float32)
            if h == bands - 1:
                acc += jnp.dot(after, pick_first, preferred_element_type=jnp.float32)
            out[q * bands + h] = acc.astype(jnp.bfloat16)
        return carry

    lax.fori_loop(0, len(slabs), slab, 0)


def spread_weights(slabs, width, bands, mem_index):
    rows, cols = slabs[0].shape
    return pl.pallas_call(
        functools.partial(spread_body, width, bands),
        out_shape=jax.ShapeDtypeStruct((len(slabs) * bands, rows, 2 * LANES), jnp.bfloat16),
        in_specs=[pl.BlockSpec(memory_space=SMEM)] + [pl.BlockSpec(memory_space=ANY)] * len(slabs),
        out_specs=pl.BlockSpec(memory_space=VMEM),
        scratch_shapes=[
            VMEM((len(slabs), rows, cols), jnp.bfloat16),
            pltpu.SemaphoreType.DMA((len(slabs),)),
        ],
        name="spread_weights",
    )(mem_index, *slabs)


def lon_body(masks, first, pairs, rows, lat_ref, control, weights, *refs):
    outs = refs[: len(masks)]
    fields_here, held, sems = refs[len(masks) :]
    here = lat_ref[0]
    members = control.shape[0]
    source = control.at[:, pl.ds(first * rows, 2 * pairs * rows), :]
    copies = copy_all(
        [(source, fields_here)]
        + [(weights.at[here ^ s], held.at[i]) for i, s in enumerate(masks)],
        sems,
    )
    copies[0].wait()
    low = lax.broadcasted_iota(jnp.int32, (rows, LANES), 1) < HALF
    for i, out in enumerate(outs):
        copies[1 + i].wait()
        for m in range(members):
            acc = jnp.dot(fields_here[m], held[i], preferred_element_type=jnp.float32)
            for p in range(pairs):
                one = acc[2 * p * rows : (2 * p + 1) * rows]
                two = acc[(2 * p + 1) * rows : (2 * p + 2) * rows]
                out[p, m, 0] = one[:, :LANES].astype(jnp.bfloat16)
                out[p, m, 1] = two[:, :LANES].astype(jnp.bfloat16)
                out[p, m, 2] = jnp.where(low, one[:, LANES:], two[:, LANES:]).astype(jnp.bfloat16)


def lon_blocks(control, weights, lat_index, masks, first, pairs, rows):
    members, _, nlon = control.shape
    block = jax.ShapeDtypeStruct((pairs, members, 3, rows, LANES), jnp.bfloat16)
    flops = 2 * members * 2 * pairs * rows * nlon * 2 * LANES * len(masks)
    return pl.pallas_call(
        functools.partial(lon_body, masks, first, pairs, rows),
        out_shape=[block] * len(masks),
        in_specs=[
            pl.BlockSpec(memory_space=SMEM),
            pl.BlockSpec(memory_space=ANY),
            pl.BlockSpec(memory_space=ANY),
        ],
        out_specs=[pl.BlockSpec(memory_space=VMEM)] * len(masks),
        scratch_shapes=[
            VMEM((members, 2 * pairs * rows, nlon), jnp.bfloat16),
            VMEM((len(masks), nlon, 2 * LANES), jnp.bfloat16),
            pltpu.SemaphoreType.DMA((1 + len(masks),)),
        ],
        cost_estimate=pl.CostEstimate(
            flops=flops, transcendentals=0, bytes_accessed=len(masks) * nlon * 4 * LANES
        ),
        name="lon_blocks",
    )(lat_index, control, weights)


def lat_body(first, pairs, width, scale, n_lat, n_mem, lat_ref, mem_ref, *refs):
    blocks = refs[:n_lat]
    slabs = refs[n_lat : n_lat + n_mem]
    perturb = refs[n_lat + n_mem]
    before, after = refs[n_lat + n_mem + 1 : n_lat + n_mem + 3]
    outs = refs[n_lat + n_mem + 3 : n_lat + 2 * n_mem + 3]
    weights, banded, pert, total, rims, sems, pair_sems = refs[n_lat + 2 * n_mem + 3 :]
    here = lat_ref[0]
    mem_here = mem_ref[0]
    rows = blocks[0].shape[3]
    rows_own, nlat = slabs[0].shape
    members = pert.shape[0]
    copies = copy_all(
        [
            (b, banded.at[:, :, :, pl.ds(pl.multiple_of((here ^ s) * rows, 8), rows), :])
            for s, b in enumerate(blocks)
        ]
        + [
            (w, weights.at[pl.ds(pl.multiple_of((mem_here ^ r) * rows_own, 8), rows_own), :])
            for r, w in enumerate(slabs)
        ],
        sems,
    )
    pair_copies = copy_all(
        [
            (perturb.at[:, pl.ds(first + 2 * p, 2)], pert.at[:, pl.ds(2 * p, 2)])
            for p in range(pairs)
        ],
        pair_sems,
    )
    count = before.shape[0]
    spot = jnp.where(
        lax.broadcasted_iota(jnp.int32, (count, LANES), 0)
        == lax.broadcasted_iota(jnp.int32, (count, LANES), 1),
        1.0,
        0.0,
    ).astype(jnp.bfloat16)
    for h, edge in enumerate((after, before)):
        rims[:, h * LANES : (h + 1) * LANES] = lax.dot_general(
            edge[...], spot, (((0,), (0,)), ((), ())), preferred_element_type=jnp.float32
        ).astype(jnp.bfloat16)
    rim_lane = lax.broadcasted_iota(jnp.int32, (2 * LANES, LANES), 0)
    own_lane = lax.broadcasted_iota(jnp.int32, (2 * LANES, LANES), 1)
    half_lane = own_lane % HALF
    late = half_lane >= HALF - STEPS
    cell = jnp.where(late, half_lane - (HALF - STEPS), half_lane - (width - LANES))
    at_rim = late | ((cell >= 0) & (cell < STEPS))
    rim_base = jnp.where(late, LANES, 0) + cell * members
    for c in copies:
        c.wait()
    for c in pair_copies:
        c.wait()
    k = lax.broadcasted_iota(jnp.int32, (width, LANES), 0)
    n = lax.broadcasted_iota(jnp.int32, (width, LANES), 1)
    picks = [
        jnp.where((k == n - h * HALF + LANES) & (n >= h * HALF), 1.0, 0.0).astype(jnp.bfloat16)
        for h in range(2)
    ]

    halo = (total.shape[0] - nlat) // 2
    total[:halo] = jnp.zeros((halo, LANES), jnp.float32)
    total[halo + nlat :] = jnp.zeros((halo, LANES), jnp.float32)

    def pair(p, carry):
        for t in range(3):
            both = jnp.concatenate([banded[p, m, t] for m in range(members)], axis=1)
            local = jnp.dot(weights[...], both, preferred_element_type=jnp.float32)
            acc = None
            for m in range(members):
                if t < 2:
                    factor = pert[m, 2 * p + t, :, :LANES].astype(jnp.float32)
                else:
                    factor = jnp.dot(
                        pert[m, 2 * p], picks[0], preferred_element_type=jnp.float32
                    ) + jnp.dot(pert[m, 2 * p + 1], picks[1], preferred_element_type=jnp.float32)
                    field = first + 2 * p + own_lane // HALF
                    pick = at_rim & (rim_lane == rim_base + field * STEPS * members + m)
                    factor += jnp.dot(
                        rims[...],
                        jnp.where(pick, 1.0, 0.0).astype(jnp.bfloat16),
                        preferred_element_type=jnp.float32,
                    )
                term = local[:, m * LANES : (m + 1) * LANES] * factor
                acc = term if acc is None else acc + term
            total[halo : halo + nlat] = acc * scale
            for r in range(n_mem):
                start = pl.multiple_of((mem_here ^ r) * rows_own, 8)
                part = total[pl.ds(start, rows_own + 2 * halo), :]
                outs[r][p, t] = part.astype(outs[r].dtype)
        return carry

    lax.fori_loop(0, pairs, pair, 0)


def lat_products(blocks, slabs, perturb, edges, lat_index, mem_index, first, scale):
    pairs, members, _, _, _ = blocks[0].shape
    n_lat, n_mem = len(blocks), len(slabs)
    rows_own, nlat = slabs[0].shape
    width = perturb.shape[3]
    own = jax.ShapeDtypeStruct((pairs, 3, rows_own + 2 * HALO, LANES), jnp.float32)
    sent = jax.ShapeDtypeStruct((pairs, 3, rows_own + 2 * HALO, LANES), jnp.bfloat16)
    return pl.pallas_call(
        functools.partial(lat_body, first, pairs, width, scale, n_lat, n_mem),
        out_shape=[own] + [sent] * (n_mem - 1),
        in_specs=[pl.BlockSpec(memory_space=SMEM)] * 2
        + [pl.BlockSpec(memory_space=ANY)] * (n_lat + n_mem + 1)
        + [pl.BlockSpec(memory_space=VMEM)] * 2,
        out_specs=[pl.BlockSpec(memory_space=VMEM)] * n_mem,
        scratch_shapes=[
            VMEM((nlat, nlat), jnp.bfloat16),
            VMEM((pairs, members, 3, nlat, LANES), jnp.bfloat16),
            VMEM((members, 2 * pairs, nlat, width), jnp.bfloat16),
            VMEM((nlat + 2 * HALO, LANES), jnp.float32),
            VMEM((nlat, 2 * LANES), jnp.bfloat16),
            pltpu.SemaphoreType.DMA((n_lat + n_mem,)),
            pltpu.SemaphoreType.DMA((pairs,)),
        ],
        cost_estimate=pl.CostEstimate(
            flops=2 * nlat * nlat * members * pairs * 3 * LANES,
            transcendentals=0,
            bytes_accessed=members * 2 * pairs * nlat * 4 * width,
        ),
        name="lat_products",
    )(lat_index, mem_index, *blocks, *slabs, perturb, *edges)


def advance_body(first, pairs, width, n_mem, aliased, *refs):
    parts = refs[:n_mem]
    background, courant = refs[n_mem : n_mem + 2]
    outs = refs[n_mem + 2 + aliased : n_mem + 4 + aliased]
    ground, wind, made, one, two, sems = refs[n_mem + 4 + aliased :]
    rows_ext = wind.shape[1]
    rows_own = rows_ext - 2 * HALO
    copies = copy_all([(courant, wind.at[pl.ds(0, 2)]), (background.at[pl.ds(first, 2 * pairs)], ground)], sems)
    low = lax.broadcasted_iota(jnp.int32, (rows_ext, LANES), 1) < HALF
    for buf in (one, two):
        buf[:HALO] = jnp.zeros((HALO, 2 * LANES), jnp.float32)
        buf[HALO + rows_ext :] = jnp.zeros((HALO, 2 * LANES), jnp.float32)
    for c in copies:
        c.wait()
    u, v = (wind[0], wind[1])
    west, east = (jnp.maximum(u, 0.0), -jnp.minimum(u, 0.0))
    south, north = (jnp.maximum(v, 0.0), -jnp.minimum(v, 0.0))
    wind[0] = 1.0 - west - east - south - north
    for i, w in enumerate((west, east, south, north)):
        wind[1 + i] = w
    block = 32

    def pair(p, carry):
        tiles = []
        for t in range(3):
            acc = parts[0][p, t]
            for part in parts[1:]:
                acc = acc + part[p, t].astype(jnp.float32)
            tiles.append(acc)
        turned = pltpu.roll(tiles[2], HALF, 1)
        tails = [jnp.where(low, tiles[2], turned), jnp.where(low, turned, tiles[2])]
        for h in range(2):
            f = 2 * p + h
            one[HALO : HALO + rows_ext, :LANES] = tiles[h] + ground[f, :, :LANES]
            one[HALO : HALO + rows_ext, LANES:] = tails[h] + ground[f, :, LANES:]
            made[0, f] = one[2 * HALO : 2 * HALO + rows_own, :width]
            bufs = (one, two)
            for step in range(STEPS):
                src, dst = (bufs[step % 2], bufs[1 - step % 2])
                for start in range(0, rows_ext, block):
                    r = pl.ds(start, block)
                    c = src[pl.ds(start + HALO, block), :]
                    new = wind[0, r, :] * c
                    new += wind[1, r, :] * pltpu.roll(c, 1, 1)
                    new += wind[2, r, :] * pltpu.roll(c, 2 * LANES - 1, 1)
                    new += wind[3, r, :] * src[pl.ds(start + HALO - 1, block), :]
                    new += wind[4, r, :] * src[pl.ds(start + HALO + 1, block), :]
                    dst[pl.ds(start + HALO, block), :] = new
            made[1, f] = bufs[STEPS % 2][2 * HALO : 2 * HALO + rows_own, :width]
        return carry

    lax.fori_loop(0, pairs, pair, 0)
    copies = copy_all(
        [(made.at[i], out.at[pl.ds(first, 2 * pairs)]) for i, out in enumerate(outs)], sems
    )
    for c in copies:
        c.wait()


def advance(parts, background, courant, shape, first, pairs, before):
    n_mem = len(parts)
    _, rows_own, width = shape
    rows_ext = background.shape[1]
    out = jax.ShapeDtypeStruct(shape, jnp.float32)
    return pl.pallas_call(
        functools.partial(advance_body, first, pairs, width, n_mem, len(before)),
        out_shape=[out, out],
        in_specs=[pl.BlockSpec(memory_space=VMEM)] * n_mem
        + [pl.BlockSpec(memory_space=ANY)] * (2 + len(before)),
        out_specs=[pl.BlockSpec(memory_space=ANY)] * 2,
        input_output_aliases={n_mem + 2 + i: i for i in range(len(before))},
        scratch_shapes=[
            VMEM((2 * pairs, rows_ext, 2 * LANES), jnp.float32),
            VMEM((5, rows_ext, 2 * LANES), jnp.float32),
            VMEM((2, 2 * pairs, rows_own, width), jnp.float32),
            VMEM((rows_ext + 2 * HALO, 2 * LANES), jnp.float32),
            VMEM((rows_ext + 2 * HALO, 2 * LANES), jnp.float32),
            pltpu.SemaphoreType.DMA((2,)),
        ],
        name="advance",
    )(*parts, background, courant, *before)


def rim(values, axis, dim, width, wrap):
    size, length = (lax.axis_size(axis), values.shape[dim])
    up = [(i, (i + 1) % size) for i in range(size if wrap else size - 1)]
    down = [(j, i) for i, j in up]
    last = lax.slice_in_dim(values, length - width, length, axis=dim)
    leading = lax.slice_in_dim(values, 0, width, axis=dim)
    return (lax.ppermute(last, axis, up), lax.ppermute(leading, axis, down))


def with_lon_rim(values, width, total):
    before, after = rim(values, "lat", values.ndim - 1, STEPS, True)
    gap = jnp.zeros(values.shape[:-1] + (total - width - 2 * STEPS,), values.dtype)
    return jnp.concatenate([values, after, gap, before], axis=-1)


def chunks_of(fields):
    plan, first = ([], 0)
    left = fields // 2
    while left:
        pairs = min(2, left)
        plan.append((first, pairs))
        first, left = (first + 2 * pairs, left - pairs)
    return plan


FAR = (6, 7, 4, 5)
NEAR = (2, 3, 1, 0)


def gate_body(mem_ref, out):
    out[0] = mem_ref[0]


def gate(mem_index):
    return pl.pallas_call(
        gate_body,
        out_shape=jax.ShapeDtypeStruct((1,), jnp.int32),
        in_specs=[pl.BlockSpec(memory_space=SMEM)],
        out_specs=pl.BlockSpec(memory_space=SMEM),
        name="gate",
    )(mem_index)


def per_device_banded(control, perturb, lon_loc, lat_loc, static_scale, static_field, courant):
    n_mem, n_lat = (lax.axis_size("mem"), lax.axis_size("lat"))
    members, fields, rows, nlon = control.shape
    width = perturb.shape[3]
    mem_index = lax.axis_index("mem").astype(jnp.int32).reshape(1)
    lat_index = lax.axis_index("lat").astype(jnp.int32).reshape(1)
    scale = 1.0 / math.sqrt(members * n_mem - 1)
    chunks = chunks_of(fields)

    lon_by_mask = {0: lon_loc}
    for bit in reversed(range(n_mem.bit_length() - 1)):
        for have in list(lon_by_mask):
            lon_by_mask[have ^ (1 << bit)] = xor_permute(lon_by_mask[have], "mem", 1 << bit)
    lon_slabs = [lon_by_mask[r] for r in range(n_mem)]
    lat_slabs = [lat_loc] + [xor_permute(lat_loc, "mem", r) for r in range(1, n_mem)]
    weights = spread_weights(lon_slabs, width, n_lat // n_mem, mem_index)

    turned = jnp.transpose(perturb, (1, 3, 0, 2))
    edges = rim(turned, "lat", 1, STEPS, True)

    product = static_scale * static_field
    ground = with_lon_rim(jnp.concatenate([product, courant], axis=0), width, 2 * LANES)
    above, below = rim(ground, "mem", 1, HALO, False)
    ground = jnp.concatenate([above, ground, below], axis=1)
    background, winds = (ground[:fields], ground[fields:])

    flat = control.reshape(members, fields * rows, nlon)
    received = []
    for c, (first, pairs) in enumerate(chunks):
        groups = {"a": FAR, "b": NEAR} if c == 0 else {"": FAR + NEAR}
        by_mask = {}
        for masks in groups.values():
            blocks = lon_blocks(flat, weights, lat_index, masks, first, pairs, rows)
            by_mask.update(zip(masks, blocks))
        arrived = {0: by_mask[0]}
        for s in FAR + NEAR:
            if s:
                arrived[s] = xor_permute(by_mask[s], "lat", s)
        received.append([arrived[s] for s in range(n_lat)])

    opened = gate(mem_index)
    perturb, edges, mem_index = lax.optimization_barrier((perturb, edges, opened))
    edges = [e.reshape(-1, e.shape[3]) for e in edges]
    outs = ()
    for (first, pairs), blocks in zip(chunks, received):
        made = lat_products(blocks, lat_slabs, perturb, edges, lat_index, mem_index, first, scale)
        parts = [made[0]]
        for r in range(1, n_mem):
            parts.append(xor_permute(made[r], "mem", r))
        outs = advance(parts, background, winds, static_scale.shape, first, pairs, outs)
    return tuple(outs)


def per_device(control, perturb, *rest):
    n_mem, n_lat = (lax.axis_size("mem"), lax.axis_size("lat"))
    rows = control.shape[2]
    width = perturb.shape[3]
    nlat = perturb.shape[2]
    banded = (
        LANES < width <= LANES + HALF - 2 * STEPS
        and rows % 8 == 0
        and (nlat // n_mem) % 8 == 0
        and control.shape[1] % 2 == 0
        and control.shape[0] * control.shape[1] * STEPS <= LANES
        and n_lat == len(FAR + NEAR)
        and n_lat % n_mem == 0
    )
    if not banded:
        return per_device_any(control, perturb, *rest)
    return per_device_banded(control, perturb, *rest)


def solution(mesh):
    placed = (
        P("mem", None, "lat", None),
        P("mem", None, None, "lat"),
        P(None, "mem"),
        P("mem", None),
        P(None, "mem", "lat"),
        P(None, "mem", "lat"),
        P(None, "mem", "lat"),
    )
    return jax.shard_map(
        per_device,
        mesh=mesh,
        in_specs=placed,
        out_specs=(P(None, "mem", "lat"), P(None, "mem", "lat")),
        check_vma=False,
    )
```

```python
import functools
import math

import jax
import jax.numpy as jnp
from jax import lax
from jax.experimental import pallas as pl
from jax.experimental.pallas import tpu as pltpu
from jax.sharding import PartitionSpec as P


STEPS = 4
LANES = 128
HALF = 64
HALO = 8
ANY = pl.ANY
SMEM = pltpu.SMEM
VMEM = pltpu.VMEM


def padded_2(shard, sides, width, wrap):
    for axis, dim in sides:
        size, length = (lax.axis_size(axis), shard.shape[dim])
        up = [(i, (i + 1) % size) for i in range(size if wrap else size - 1)]
        down = [(j, i) for i, j in up]
        last = lax.slice_in_dim(shard, length - width, length, axis=dim)
        leading = lax.slice_in_dim(shard, 0, width, axis=dim)
        before = lax.ppermute(last, axis, up)
        after = lax.ppermute(leading, axis, down)
        shard = jnp.concatenate([before, shard, after], axis=dim)
    return shard


def upwind(padded, east_west, north_south):
    center = padded[:, 1:-1, 1:-1]
    western = padded[:, 1:-1, :-2]
    eastern = padded[:, 1:-1, 2:]
    southern = padded[:, :-2, 1:-1]
    northern = padded[:, 2:, 1:-1]
    zonal = jnp.maximum(east_west, 0.0) * (center - western) + jnp.minimum(east_west, 0.0) * (
        eastern - center
    )
    meridional = jnp.maximum(north_south, 0.0) * (center - southern) + jnp.minimum(
        north_south, 0.0
    ) * (northern - center)
    return center - zonal - meridional


def evolve(current, courant):
    fields = current.shape[0]
    stacked = jnp.concatenate([current, courant], axis=0)
    extended = padded_2(stacked, (("lat", 2),), STEPS, True)
    extended = padded_2(extended, (("mem", 1),), STEPS, False)
    result = extended[:fields]
    wind_ext = extended[fields:]
    for step_index in range(STEPS):
        margin = step_index + 1
        inner_wind = wind_ext[
            :, margin : wind_ext.shape[1] - margin, margin : wind_ext.shape[2] - margin
        ]
        result = upwind(result, inner_wind[0], inner_wind[1])
    return result


def per_device_any(control, perturb, lon_loc, lat_loc, static_scale, static_field, courant):
    along_lon = jnp.einsum(
        "mfal,lc->amfc",
        control,
        lax.all_gather(lon_loc, "mem", axis=1, tiled=True),
        preferred_element_type=jnp.float32,
    ).astype(jnp.bfloat16)
    banded = lax.all_to_all(along_lon, "lat", split_axis=3, concat_axis=0, tiled=True)
    nlat = banded.shape[0]
    mem_here = banded.shape[1]
    fields = banded.shape[2]
    lon_width = banded.shape[3]
    flat_band = banded.reshape(nlat, mem_here * fields * lon_width)
    pert_rows = jnp.transpose(perturb, (2, 0, 1, 3))
    lat_weights_all = lax.all_gather(lat_loc, "mem", axis=0, tiled=True)
    members = mem_here * lax.axis_size("mem")
    ens_scale = 1.0 / math.sqrt(members - 1)
    rows_own = nlat // lax.axis_size("mem")
    localized = jnp.dot(lat_weights_all, flat_band, preferred_element_type=jnp.float32)
    localized = localized.reshape(nlat, mem_here, fields, lon_width)
    ensemble_all = jnp.transpose(
        lax.psum(jnp.sum(localized * pert_rows.astype(jnp.float32), axis=1) * ens_scale, "mem"),
        (1, 0, 2),
    )
    offset = lax.axis_index("mem") * rows_own
    ensemble = lax.dynamic_slice_in_dim(ensemble_all, offset, rows_own, 1)
    increment = ensemble + static_scale * static_field
    evolved = evolve(increment, courant)
    return (increment, evolved)


def xor_permute(value, axis, mask):
    return lax.ppermute(value, axis, [(i, i ^ mask) for i in range(lax.axis_size(axis))])


def copy_all(pairs, sems):
    copies = [pltpu.make_async_copy(a, b, sems.at[i]) for i, (a, b) in enumerate(pairs)]
    for c in copies:
        c.start()
    return copies


def spread_matrix(width, rows, first):
    k = lax.broadcasted_iota(jnp.int32, (rows, 4 * LANES), 0)
    lane = lax.broadcasted_iota(jnp.int32, (rows, 4 * LANES), 1)
    n = lane % (2 * LANES)
    n = jnp.where(n >= LANES + HALF, n - HALF, n)
    late = n >= LANES + HALF - STEPS
    column = jnp.where(late, n - LANES - HALF, n) + lane // (2 * LANES) * width
    taken = late | (n < width + STEPS)
    return jnp.where(taken & (k + first == column), 1.0, 0.0).astype(jnp.bfloat16)


def lon_first_body(masks, first, pairs, rows, width, lat_ref, mem_ref, control, *refs):
    count = len(refs) - len(masks) - 6
    slabs = refs[:count]
    outs = refs[count : count + len(masks)]
    kept, fields_here, slab_held, held, sems, kept_sems = refs[count + len(masks) :]
    here = lat_ref[0]
    mem_here = mem_ref[0]
    source = control.at[:, pl.ds(first * rows, 2 * pairs * rows), :]
    copies = copy_all(
        [(s, slab_held.at[mem_here ^ r]) for r, s in enumerate(slabs)] + [(source, fields_here)],
        sems,
    )
    _, _, cols = slab_held.shape
    split = 2 * LANES
    pick_low = spread_matrix(width, split, 0)
    pick_high = spread_matrix(width, cols - split, split)
    pick_before = spread_matrix(width, cols - split, split - cols)
    pick_after = spread_matrix(width, LANES, cols)
    for c in copies:
        c.wait()
    kept_copies = []
    for i in range(0, len(masks), 2):
        q = (here ^ masks[i]) // 2
        parts = (
            (slab_held[q, :, :split], pick_low),
            (slab_held[q, :, split:], pick_high),
            (slab_held[(q + count - 1) % count, :, split:], pick_before),
            (slab_held[(q + 1) % count, :, :LANES], pick_after),
        )
        acc = sum(jnp.dot(x, y, preferred_element_type=jnp.float32) for x, y in parts)
        for h in range(2):
            slot = i + ((here ^ masks[i] ^ h) & 1)
            held[slot] = acc[:, h * 2 * LANES : (h + 1) * 2 * LANES].astype(jnp.bfloat16)
        for k in range(i, i + 2):
            c = pltpu.make_async_copy(held.at[k], kept.at[k], kept_sems.at[k])
            c.start()
            kept_copies.append(c)
            lon_tiles(fields_here, held[k], outs[k], pairs, rows)
    for c in kept_copies:
        c.wait()


def lon_first(control, slabs, lat_index, mem_index, masks, first, pairs, rows, width):
    members, _, nlon = control.shape
    block = jax.ShapeDtypeStruct((pairs, members, 3, rows, LANES), jnp.bfloat16)
    kept = jax.ShapeDtypeStruct((len(masks), nlon, 2 * LANES), jnp.bfloat16)
    return pl.pallas_call(
        functools.partial(lon_first_body, masks, first, pairs, rows, width),
        out_shape=[block] * len(masks) + [kept],
        in_specs=[pl.BlockSpec(memory_space=SMEM)] * 2
        + [pl.BlockSpec(memory_space=ANY)] * (1 + len(slabs)),
        out_specs=[pl.BlockSpec(memory_space=VMEM)] * len(masks)
        + [pl.BlockSpec(memory_space=ANY)],
        scratch_shapes=[
            VMEM((members, 2 * pairs * rows, nlon), jnp.bfloat16),
            VMEM((len(slabs),) + slabs[0].shape, jnp.bfloat16),
            VMEM(kept.shape, jnp.bfloat16),
            pltpu.SemaphoreType.DMA((1 + len(slabs),)),
            pltpu.SemaphoreType.DMA((len(masks),)),
        ],
        name="lon_first",
    )(lat_index, mem_index, control, *slabs)


def lon_tiles(fields_here, weights, out, pairs, rows):
    low = lax.broadcasted_iota(jnp.int32, (rows, LANES), 1) < HALF
    for m in range(fields_here.shape[0]):
        acc = jnp.dot(fields_here[m], weights, preferred_element_type=jnp.float32)
        for p in range(pairs):
            one = acc[2 * p * rows : (2 * p + 1) * rows]
            two = acc[(2 * p + 1) * rows : (2 * p + 2) * rows]
            out[p, m, 0] = one[:, :LANES].astype(jnp.bfloat16)
            out[p, m, 1] = two[:, :LANES].astype(jnp.bfloat16)
            out[p, m, 2] = jnp.where(low, one[:, LANES:], two[:, LANES:]).astype(jnp.bfloat16)


def lon_body(first, pairs, rows, groups, control, *refs):
    kept = [g.at[i] for g in refs[:groups] for i in range(g.shape[0])]
    outs = refs[groups : groups + len(kept)]
    fields_here, held, sems = refs[groups + len(kept) :]
    source = control.at[:, pl.ds(first * rows, 2 * pairs * rows), :]
    copies = copy_all(
        [(source, fields_here)] + [(w, held.at[i]) for i, w in enumerate(kept)], sems
    )
    copies[0].wait()
    for i, out in enumerate(outs):
        copies[1 + i].wait()
        lon_tiles(fields_here, held[i], out, pairs, rows)


def lon_blocks(control, kept, first, pairs, rows):
    members, _, nlon = control.shape
    count = sum(g.shape[0] for g in kept)
    block = jax.ShapeDtypeStruct((pairs, members, 3, rows, LANES), jnp.bfloat16)
    return pl.pallas_call(
        functools.partial(lon_body, first, pairs, rows, len(kept)),
        out_shape=[block] * count,
        in_specs=[pl.BlockSpec(memory_space=ANY)] * (1 + len(kept)),
        out_specs=[pl.BlockSpec(memory_space=VMEM)] * count,
        scratch_shapes=[
            VMEM((members, 2 * pairs * rows, nlon), jnp.bfloat16),
            VMEM((count, nlon, 2 * LANES), jnp.bfloat16),
            pltpu.SemaphoreType.DMA((1 + count,)),
        ],
        cost_estimate=pl.CostEstimate(
            flops=2 * members * 2 * pairs * rows * nlon * 2 * LANES * count,
            transcendentals=0,
            bytes_accessed=count * nlon * 4 * LANES,
        ),
        name="lon_blocks",
    )(control, *kept)


def lat_body(first, pairs, width, scale, n_lat, n_mem, lat_ref, mem_ref, *refs):
    blocks = refs[:n_lat]
    slabs = refs[n_lat : n_lat + n_mem]
    perturb = refs[n_lat + n_mem]
    rim_sources = refs[n_lat + n_mem + 1 : n_lat + n_mem + 3]
    results = refs[n_lat + n_mem + 3 : n_lat + 2 * n_mem + 3]
    scratch = refs[n_lat + 2 * n_mem + 3 :]
    outs = scratch[:n_mem]
    weights, banded, pert, total, rims, edges = scratch[n_mem : n_mem + 6]
    sems, pair_sems, out_sems = scratch[n_mem + 6 :]
    here = lat_ref[0]
    mem_here = mem_ref[0]
    rows = blocks[0].shape[3]
    rows_own, nlat = slabs[0].shape
    members = pert.shape[0]
    copies = copy_all(
        [(e, edges.at[h]) for h, e in enumerate(rim_sources)]
        + [
            (w, weights.at[pl.ds(pl.multiple_of((mem_here ^ r) * rows_own, 8), rows_own), :])
            for r, w in enumerate(slabs)
        ],
        sems,
    )
    pair_copies = []
    for p in range(pairs):
        moves = [
            (b.at[p], banded.at[p, :, :, pl.ds(pl.multiple_of((here ^ s) * rows, 8), rows), :])
            for s, b in enumerate(blocks)
        ]
        moves.append((perturb.at[:, pl.ds(first + 2 * p, 2)], pert.at[:, pl.ds(2 * p, 2)]))
        pair_copies.append(copy_all(moves, pair_sems.at[p]))
    count = edges.shape[1]
    spot = jnp.where(
        lax.broadcasted_iota(jnp.int32, (count, LANES), 0)
        == lax.broadcasted_iota(jnp.int32, (count, LANES), 1),
        1.0,
        0.0,
    ).astype(jnp.bfloat16)
    for c in copies:
        c.wait()
    for h in range(2):
        rims[:, (1 - h) * LANES : (2 - h) * LANES] = lax.dot_general(
            edges[h], spot, (((0,), (0,)), ((), ())), preferred_element_type=jnp.float32
        ).astype(jnp.bfloat16)
    rim_lane = lax.broadcasted_iota(jnp.int32, (2 * LANES, LANES), 0)
    own_lane = lax.broadcasted_iota(jnp.int32, (2 * LANES, LANES), 1)
    half_lane = own_lane % HALF
    late = half_lane >= HALF - STEPS
    cell = jnp.where(late, half_lane - (HALF - STEPS), half_lane - (width - LANES))
    at_rim = late | ((cell >= 0) & (cell < STEPS))
    rim_base = jnp.where(late, LANES, 0) + cell * members
    k = lax.broadcasted_iota(jnp.int32, (width, LANES), 0)
    n = lax.broadcasted_iota(jnp.int32, (width, LANES), 1)
    picks = [
        jnp.where((k == n - h * HALF + LANES) & (n >= h * HALF), 1.0, 0.0).astype(jnp.bfloat16)
        for h in range(2)
    ]

    halo = (total.shape[0] - nlat) // 2
    total[:halo] = jnp.zeros((halo, LANES), jnp.float32)
    total[halo + nlat :] = jnp.zeros((halo, LANES), jnp.float32)

    out_copies = []
    for p in range(pairs):
        for c in pair_copies[p]:
            c.wait()
        for t in range(3):
            both = jnp.concatenate([banded[p, m, t] for m in range(members)], axis=1)
            local = jnp.dot(weights[...], both, preferred_element_type=jnp.float32)
            acc = None
            for m in range(members):
                if t < 2:
                    factor = pert[m, 2 * p + t, :, :LANES].astype(jnp.float32)
                else:
                    factor = jnp.dot(
                        pert[m, 2 * p], picks[0], preferred_element_type=jnp.float32
                    ) + jnp.dot(pert[m, 2 * p + 1], picks[1], preferred_element_type=jnp.float32)
                    field = first + 2 * p + own_lane // HALF
                    pick = at_rim & (rim_lane == rim_base + field * STEPS * members + m)
                    factor += jnp.dot(
                        rims[...],
                        jnp.where(pick, 1.0, 0.0).astype(jnp.bfloat16),
                        preferred_element_type=jnp.float32,
                    )
                term = local[:, m * LANES : (m + 1) * LANES] * factor
                acc = term if acc is None else acc + term
            total[halo : halo + nlat] = acc * scale
            for r in range(n_mem):
                start = pl.multiple_of((mem_here ^ r) * rows_own, 8)
                part = total[pl.ds(start, rows_own + 2 * halo), :]
                outs[r][p, t] = part.astype(outs[r].dtype)
        out_copies += copy_all(
            [(o.at[p], result.at[p]) for o, result in zip(outs, results)], out_sems.at[p]
        )
    for c in out_copies:
        c.wait()


def lat_products(blocks, slabs, perturb, edges, lat_index, mem_index, first, scale):
    pairs, members, _, _, _ = blocks[0].shape
    n_lat, n_mem = len(blocks), len(slabs)
    rows_own, nlat = slabs[0].shape
    width = perturb.shape[3]
    own = jax.ShapeDtypeStruct((pairs, 3, rows_own + 2 * HALO, LANES), jnp.float32)
    sent = jax.ShapeDtypeStruct((pairs, 3, rows_own + 2 * HALO, LANES), jnp.bfloat16)
    return pl.pallas_call(
        functools.partial(lat_body, first, pairs, width, scale, n_lat, n_mem),
        out_shape=[own] + [sent] * (n_mem - 1),
        in_specs=[pl.BlockSpec(memory_space=SMEM)] * 2
        + [pl.BlockSpec(memory_space=ANY)] * (n_lat + n_mem + 3),
        out_specs=[pl.BlockSpec(memory_space=ANY)] * n_mem,
        scratch_shapes=[VMEM(o.shape, o.dtype) for o in [own] + [sent] * (n_mem - 1)]
        + [
            VMEM((nlat, nlat), jnp.bfloat16),
            VMEM((pairs, members, 3, nlat, LANES), jnp.bfloat16),
            VMEM((members, 2 * pairs, nlat, width), jnp.bfloat16),
            VMEM((nlat + 2 * HALO, LANES), jnp.float32),
            VMEM((nlat, 2 * LANES), jnp.bfloat16),
            VMEM((2,) + edges[0].shape, jnp.bfloat16),
            pltpu.SemaphoreType.DMA((n_mem + 2,)),
            pltpu.SemaphoreType.DMA((pairs, n_lat + 1)),
            pltpu.SemaphoreType.DMA((pairs, n_mem)),
        ],
        cost_estimate=pl.CostEstimate(
            flops=2 * nlat * nlat * members * pairs * 3 * LANES,
            transcendentals=0,
            bytes_accessed=members * 2 * pairs * nlat * 4 * width,
        ),
        name="lat_products",
    )(lat_index, mem_index, *blocks, *slabs, perturb, *edges)


def advance_body(first, pairs, width, n_mem, aliased, *refs):
    parts = refs[:n_mem]
    background, courant = refs[n_mem : n_mem + 2]
    outs = refs[n_mem + 2 + aliased : n_mem + 4 + aliased]
    ground, wind, made, one, two, sems = refs[n_mem + 4 + aliased :]
    rows_ext = wind.shape[1]
    rows_own = rows_ext - 2 * HALO
    copies = copy_all([(courant, wind.at[pl.ds(0, 2)]), (background.at[pl.ds(first, 2 * pairs)], ground)], sems)
    low = lax.broadcasted_iota(jnp.int32, (rows_ext, LANES), 1) < HALF
    for buf in (one, two):
        buf[:HALO] = jnp.zeros((HALO, 2 * LANES), jnp.float32)
        buf[HALO + rows_ext :] = jnp.zeros((HALO, 2 * LANES), jnp.float32)
    for c in copies:
        c.wait()
    u, v = (wind[0], wind[1])
    west, east = (jnp.maximum(u, 0.0), -jnp.minimum(u, 0.0))
    south, north = (jnp.maximum(v, 0.0), -jnp.minimum(v, 0.0))
    wind[0] = 1.0 - west - east - south - north
    for i, w in enumerate((west, east, south, north)):
        wind[1 + i] = w
    block = 32

    def pair(p, carry):
        tiles = []
        for t in range(3):
            acc = parts[0][p, t]
            for part in parts[1:]:
                acc = acc + part[p, t].astype(jnp.float32)
            tiles.append(acc)
        turned = pltpu.roll(tiles[2], HALF, 1)
        tails = [jnp.where(low, tiles[2], turned), jnp.where(low, turned, tiles[2])]
        for h in range(2):
            f = 2 * p + h
            one[HALO : HALO + rows_ext, :LANES] = tiles[h] + ground[f, :, :LANES]
            one[HALO : HALO + rows_ext, LANES:] = tails[h] + ground[f, :, LANES:]
            made[0, f] = one[2 * HALO : 2 * HALO + rows_own, :width]
            bufs = (one, two)
            for step in range(STEPS):
                src, dst = (bufs[step % 2], bufs[1 - step % 2])
                for start in range(0, rows_ext, block):
                    r = pl.ds(start, block)
                    c = src[pl.ds(start + HALO, block), :]
                    new = wind[0, r, :] * c
                    new += wind[1, r, :] * pltpu.roll(c, 1, 1)
                    new += wind[2, r, :] * pltpu.roll(c, 2 * LANES - 1, 1)
                    new += wind[3, r, :] * src[pl.ds(start + HALO - 1, block), :]
                    new += wind[4, r, :] * src[pl.ds(start + HALO + 1, block), :]
                    dst[pl.ds(start + HALO, block), :] = new
            made[1, f] = bufs[STEPS % 2][2 * HALO : 2 * HALO + rows_own, :width]
        return carry

    lax.fori_loop(0, pairs, pair, 0)
    copies = copy_all(
        [(made.at[i], out.at[pl.ds(first, 2 * pairs)]) for i, out in enumerate(outs)], sems
    )
    for c in copies:
        c.wait()


def advance(parts, background, courant, shape, first, pairs, before):
    n_mem = len(parts)
    _, rows_own, width = shape
    rows_ext = background.shape[1]
    out = jax.ShapeDtypeStruct(shape, jnp.float32)
    return pl.pallas_call(
        functools.partial(advance_body, first, pairs, width, n_mem, len(before)),
        out_shape=[out, out],
        in_specs=[pl.BlockSpec(memory_space=VMEM)] * n_mem
        + [pl.BlockSpec(memory_space=ANY)] * (2 + len(before)),
        out_specs=[pl.BlockSpec(memory_space=ANY)] * 2,
        input_output_aliases={n_mem + 2 + i: i for i in range(len(before))},
        scratch_shapes=[
            VMEM((2 * pairs, rows_ext, 2 * LANES), jnp.float32),
            VMEM((5, rows_ext, 2 * LANES), jnp.float32),
            VMEM((2, 2 * pairs, rows_own, width), jnp.float32),
            VMEM((rows_ext + 2 * HALO, 2 * LANES), jnp.float32),
            VMEM((rows_ext + 2 * HALO, 2 * LANES), jnp.float32),
            pltpu.SemaphoreType.DMA((2,)),
        ],
        name="advance",
    )(*parts, background, courant, *before)


def rim(values, axis, dim, width, wrap):
    size, length = (lax.axis_size(axis), values.shape[dim])
    up = [(i, (i + 1) % size) for i in range(size if wrap else size - 1)]
    down = [(j, i) for i, j in up]
    last = lax.slice_in_dim(values, length - width, length, axis=dim)
    leading = lax.slice_in_dim(values, 0, width, axis=dim)
    return (lax.ppermute(last, axis, up), lax.ppermute(leading, axis, down))


def with_lon_rim(values, width, total):
    before, after = rim(values, "lat", values.ndim - 1, STEPS, True)
    gap = jnp.zeros(values.shape[:-1] + (total - width - 2 * STEPS,), values.dtype)
    return jnp.concatenate([values, after, gap, before], axis=-1)


def chunks_of(fields):
    plan, first = ([], 0)
    left = fields // 2
    while left:
        pairs = min(2, left)
        plan.append((first, pairs))
        first, left = (first + 2 * pairs, left - pairs)
    return plan


FAR = (4, 5, 6, 7)
NEAR = (2, 3, 1, 0)
FIRST = (FAR[:2], FAR[2:], NEAR)


def gate_body(mem_ref, out):
    out[0] = mem_ref[0]


def gate(mem_index):
    return pl.pallas_call(
        gate_body,
        out_shape=jax.ShapeDtypeStruct((1,), jnp.int32),
        in_specs=[pl.BlockSpec(memory_space=SMEM)],
        out_specs=pl.BlockSpec(memory_space=SMEM),
        name="gate",
    )(mem_index)


def per_device_banded(control, perturb, lon_loc, lat_loc, static_scale, static_field, courant):
    n_mem, n_lat = (lax.axis_size("mem"), lax.axis_size("lat"))
    members, fields, rows, nlon = control.shape
    width = perturb.shape[3]
    mem_index = lax.axis_index("mem").astype(jnp.int32).reshape(1)
    lat_index = lax.axis_index("lat").astype(jnp.int32).reshape(1)
    scale = 1.0 / math.sqrt(members * n_mem - 1)
    chunks = chunks_of(fields)

    lon_by_mask = {0: lon_loc}
    for bit in reversed(range(n_mem.bit_length() - 1)):
        for have in list(lon_by_mask):
            lon_by_mask[have ^ (1 << bit)] = xor_permute(lon_by_mask[have], "mem", 1 << bit)
    lon_slabs = [lon_by_mask[r] for r in range(n_mem)]
    lat_slabs = [lat_loc] + [xor_permute(lat_loc, "mem", r) for r in range(1, n_mem)]
    turned = jnp.transpose(perturb, (1, 3, 0, 2))
    edges = rim(turned, "lat", 1, STEPS, True)

    product = static_scale * static_field
    ground = with_lon_rim(jnp.concatenate([product, courant], axis=0), width, 2 * LANES)
    above, below = rim(ground, "mem", 1, HALO, False)
    ground = jnp.concatenate([above, ground, below], axis=1)
    background, winds = (ground[:fields], ground[fields:])

    flat = control.reshape(members, fields * rows, nlon)
    received = []
    kept = []
    for c, (first, pairs) in enumerate(chunks):
        if c == 0:
            by_mask = {}
            for masks in FIRST:
                made = lon_first(
                    flat, lon_slabs, lat_index, mem_index, masks, first, pairs, rows, width
                )
                by_mask.update(zip(masks, made))
                kept.append(made[-1])
        else:
            by_mask = dict(zip(FAR + NEAR, lon_blocks(flat, kept, first, pairs, rows)))
        arrived = {0: by_mask[0]}
        for s in FAR + NEAR:
            if s:
                arrived[s] = xor_permute(by_mask[s], "lat", s)
        received.append([arrived[s] for s in range(n_lat)])

    opened = gate(mem_index)
    perturb, edges, mem_index = lax.optimization_barrier((perturb, edges, opened))
    edges = [e.reshape(-1, e.shape[3]) for e in edges]
    outs = ()
    for (first, pairs), blocks in zip(chunks, received):
        made = lat_products(blocks, lat_slabs, perturb, edges, lat_index, mem_index, first, scale)
        parts = [made[0]]
        for r in range(1, n_mem):
            parts.append(xor_permute(made[r], "mem", r))
        outs = advance(parts, background, winds, static_scale.shape, first, pairs, outs)
    return tuple(outs)


def per_device(control, perturb, *rest):
    n_mem, n_lat = (lax.axis_size("mem"), lax.axis_size("lat"))
    rows = control.shape[2]
    width = perturb.shape[3]
    nlat = perturb.shape[2]
    banded = (
        LANES < width <= LANES + HALF - 2 * STEPS
        and rows % 8 == 0
        and (nlat // n_mem) % 8 == 0
        and control.shape[1] % 2 == 0
        and control.shape[0] * control.shape[1] * STEPS <= LANES
        and n_lat == len(FAR + NEAR)
        and n_lat == 2 * n_mem
        and 2 * LANES + STEPS <= 2 * width <= 2 * LANES + LANES - STEPS
    )
    if not banded:
        return per_device_any(control, perturb, *rest)
    return per_device_banded(control, perturb, *rest)


def solution(mesh):
    placed = (
        P("mem", None, "lat", None),
        P("mem", None, None, "lat"),
        P(None, "mem"),
        P("mem", None),
        P(None, "mem", "lat"),
        P(None, "mem", "lat"),
        P(None, "mem", "lat"),
    )
    return jax.shard_map(
        per_device,
        mesh=mesh,
        in_specs=placed,
        out_specs=(P(None, "mem", "lat"), P(None, "mem", "lat")),
        check_vma=False,
    )
```
